32 devices in a mesh: row: 2 (over y), col: 4 (over z), depth: 4 (over x, core).
Axes of the slice: x: 2, y: 2, z: 4, core: 2. Of those that a mesh axis runs over, the one named last changes fastest.
Arguments:
- grad_out: bfloat16 [1024, 6144], P('depth', 'col'), may hold values from -6 to 6
- pre_act: bfloat16 [1024, 24576], P('depth', 'row'), may hold values from -8 to 8
- down_weight: bfloat16 [24576, 6144], P(('row', 'depth'), 'col'), may hold values from -0.0546875 to 0.0546875
Outputs:
- grad_pre: bfloat16 [1024, 24576], P('depth', 'row')
- grad_weight: bfloat16 [24576, 6144], P(('row', 'depth'), 'col')
The draws below stay inside these ranges and needn't reach their ends.
All inputs are finite; a program needn't handle non-finite values.
Results may differ from the reference program's by a relative error of at most 0.0066.
Values may be sent and summed in bfloat16 or wider, within the bound.
A program may use at most 128 MiB of HBM per device.

```python
import jax
import jax.numpy as jnp

D = 6144
FF = 24576
TOKENS = 1024


def with_spikes(values, rng, source, target, shards_of, factor):
    owner, partner = [(jnp.arange(values.shape[dim]) // (values.shape[dim] // shards_of)).reshape([-1 if axis == dim else 1 for axis in range(values.ndim)]) for dim in (source, target)]
    chosen = jax.random.permutation(rng, shards_of)[partner]
    strong = (owner == chosen) | (owner == (partner + shards_of // 2) % shards_of)
    return jnp.where(strong, factor * values, values)


def levels(stream_key, extent, cuts, low, largest):
    gain, own = 1.0, jax.random.fold_in(stream_key, 6)
    for position, parts in cuts:
        heights = jnp.exp(jax.random.uniform(jax.random.fold_in(own, position), (parts,), jnp.float32, low / len(cuts), largest / len(cuts)))
        gain = gain * jnp.repeat(heights, extent[position] // parts).reshape([-1 if axis == position else 1 for axis in range(len(extent))])
    return gain


def scatter_about(stream_key, dims, spread, bound, shards=(), held_as=jnp.bfloat16):
    entries = spread * jax.random.normal(stream_key, dims, jnp.float32)
    if shards:
        entries = entries * levels(stream_key, dims, shards, -0.22, 0.18)
    return jnp.clip(entries, -bound, bound).astype(held_as)


def gaussian_with(key, dims, spread, reach, pieces, heavy, held_as=jnp.bfloat16):
    drawn = spread * jax.random.normal(key, dims, jnp.float32)
    if pieces:
        drawn = drawn * levels(key, dims, pieces, -0.22, 0.18)
    return jnp.clip(with_spikes(drawn, jax.random.fold_in(key, 3), *heavy), -reach, reach).astype(held_as)


def setup_inputs(seed: int = 0) -> dict:
    arg_keys = jax.random.split(jax.random.key(seed), 4)
    grad_out = scatter_about(arg_keys[0], (TOKENS, D), 1.0, 6.0, ((0, 4), (1, 4)))
    pre_act = gaussian_with(arg_keys[1], (TOKENS, FF), 1.5, 8.0, ((0, 4), (1, 2)), (0, 1, 4, 2.0))
    down_weight = gaussian_with(arg_keys[2], (FF, D), FF ** -0.5, 0.0546875, ((0, 8), (1, 4)), (1, 0, 8, 2.0))
    return dict(grad_out=grad_out, pre_act=pre_act, down_weight=down_weight)


sqrt_two_pi = 0.7978845608028654
cubic_coeff = 0.044715

def gelu_value(preact):
    tangent = jnp.tanh(sqrt_two_pi * (preact + cubic_coeff * preact * preact * preact))
    return 0.5 * preact * (1.0 + tangent)

def gelu_slope(preact):
    tangent = jnp.tanh(sqrt_two_pi * (preact + cubic_coeff * preact * preact * preact))
    inner = sqrt_two_pi * (1.0 + 3.0 * cubic_coeff * preact * preact)
    return 0.5 * (1.0 + tangent) + 0.5 * preact * (1.0 - tangent * tangent) * inner

def reference(grad_out, pre_act, down_weight):
    widened = pre_act.astype(jnp.float32)
    activation = gelu_value(widened).astype(jnp.bfloat16)
    backward = jnp.dot(grad_out, down_weight.T, preferred_element_type=jnp.float32)
    grad_pre = (backward * gelu_slope(widened)).astype(jnp.bfloat16)
    grad_weight = jnp.dot(activation.T, grad_out, preferred_element_type=jnp.float32).astype(jnp.bfloat16)
    return (grad_pre, grad_weight)
```

```python
import functools

import jax
import jax.numpy as jnp
from jax import lax
from jax.experimental import pallas as pl
from jax.experimental.pallas import tpu as pltpu
from jax.sharding import PartitionSpec as P

MESH = pl.DeviceIdType.MESH
sqrt_two_pi = 0.7978845608028654
cubic_coeff = 0.044715
LAG = 2


def gelu_value(preact):
    tangent = jnp.tanh(sqrt_two_pi * (preact + cubic_coeff * preact * preact * preact))
    return 0.5 * preact * (1.0 + tangent)


def gelu_slope(preact):
    tangent = jnp.tanh(sqrt_two_pi * (preact + cubic_coeff * preact * preact * preact))
    inner = sqrt_two_pi * (1.0 + 3.0 * cubic_coeff * preact * preact)
    return 0.5 * (1.0 + tangent) + 0.5 * preact * (1.0 - tangent * tangent) * inner


def flip(a, b, extent):
    total, k = jnp.int32(0), 1
    while k < extent:
        bit = lax.div(a, jnp.int32(k)) + lax.div(b, jnp.int32(k))
        total = total + lax.rem(bit, jnp.int32(2)) * k
        k *= 2
    return total


def kernel(
    depths, width, grad_ref, pre_ref, weight_ref, out_ref, gw_ref,
    sums, from_edge, from_middle, pre, act, out, weight, grad,
    weight_sem, pre_sem, grad_sem, edge_sem, middle_sem, swap_sem, near_sem, far_sem,
    grad_send, sums_send, relay_send, swap_send, near_send, far_send, pass_send, pre_send,
    out_sem, gw_sem,
):
    col, place = lax.axis_index("col"), lax.axis_index("depth")
    rows, hidden = grad_ref.shape[0], weight_ref.shape[0]
    half = rows // 2
    tiles = hidden // width
    total = depths * tiles
    middle = (col == 1) | (col == 2)
    edge = (col == 0) | (col == 3)
    near = col + 1 - 2 * lax.rem(col, 2)
    across = 3 - col
    mine = pl.ds(pl.multiple_of(lax.rem(col + 1, 2) * half, half), half)
    theirs = pl.ds(pl.multiple_of(lax.rem(col, 2) * half, half), half)

    def columns(block, tile):
        return pl.ds(pl.multiple_of(block * hidden + tile * width, width), width)

    def to(axis, index):
        return {axis: index}

    def send(src, dst, send_sem, recv_sem, device):
        return pltpu.make_async_remote_copy(
            src_ref=src, dst_ref=dst, send_sem=send_sem, recv_sem=recv_sem,
            device_id=device, device_id_type=MESH,
        )

    def split(q):
        return lax.div(q, jnp.int32(tiles)), lax.rem(q, jnp.int32(tiles))

    def block_rows(s):
        return pl.ds(pl.multiple_of(s * rows, rows), rows)

    def load_weight(tile):
        return pltpu.make_async_copy(
            weight_ref.at[pl.ds(pl.multiple_of(tile * width, width), width), :],
            weight.at[tile], weight_sem.at[tile],
        )

    def load_pre(tile):
        return pltpu.make_async_copy(
            pre_ref.at[:, columns(place, tile)], pre.at[0, tile], pre_sem.at[tile]
        )

    def send_pre(s, tile):
        target = flip(place, s, depths)
        return send(
            pre_ref.at[:, columns(target, tile)], pre.at[s, tile], pre_send,
            pre_sem.at[s * tiles + tile], to("depth", target),
        )

    def load_grad():
        return pltpu.make_async_copy(grad_ref, grad.at[block_rows(0)], grad_sem.at[0])

    def send_grad(s):
        return send(
            grad_ref, grad.at[block_rows(s)], grad_send.at[s], grad_sem.at[s],
            to("depth", flip(place, jnp.int32(s), depths)),
        )

    def pass_grad(s):
        return send(
            grad.at[block_rows(s)], grad.at[block_rows(s + 1)], grad_send.at[s + 1],
            grad_sem.at[s + 1], to("depth", flip(place, jnp.int32(1), depths)),
        )

    def send_sums(q):
        return send(sums.at[q], from_edge.at[q], sums_send, edge_sem.at[q], to("col", near))

    def send_relay(q):
        return send(
            sums.at[q, theirs], from_middle.at[q], relay_send, middle_sem.at[q],
            to("col", across),
        )

    def send_swap(q):
        s, tile = split(q)
        return send(
            sums.at[q, mine], out.at[place, tile, mine], swap_send, swap_sem.at[q],
            to("depth", flip(place, s, depths)),
        )

    def send_out(q, which, send_sem, recv_sem, column):
        s, tile = split(q)
        part = out.at[flip(place, s, depths), tile, which]
        return send(part, part, send_sem, recv_sem.at[q], to("col", column))

    def store_out(q):
        s, tile = split(q)
        block = flip(place, s, depths)
        return pltpu.make_async_copy(
            out.at[block, tile], out_ref.at[:, columns(block, tile)], out_sem
        )

    def store_gw(tile):
        return pltpu.make_async_copy(
            weight.at[tile],
            gw_ref.at[pl.ds(pl.multiple_of(tile * width, width), width), :], gw_sem,
        )

    load_grad().start()
    load_weight(0).start()

    barrier = pltpu.get_barrier_semaphore()
    for s in range(1, depths):
        pl.semaphore_signal(
            barrier, inc=1, device_id=to("depth", flip(place, jnp.int32(s), depths)),
            device_id_type=MESH,
        )
    pl.semaphore_signal(barrier, inc=1, device_id=to("col", near), device_id_type=MESH)

    @pl.when(middle)
    def _():
        pl.semaphore_signal(barrier, inc=1, device_id=to("col", across), device_id_type=MESH)

    @pl.loop(1, tiles)
    def _(tile):
        load_weight(tile).start()

    @pl.loop(0, tiles)
    def _(tile):
        load_pre(tile).start()

    @pl.when(middle)
    def _():
        pl.semaphore_wait(barrier, depths + 1)

    @pl.when(edge)
    def _():
        pl.semaphore_wait(barrier, depths)

    send_grad(1).start()
    for s in range(2, depths, 2):
        send_grad(s).start()
    load_grad().wait()

    step_rows = 32

    def by_rows(count, body):
        @pl.loop(0, count // step_rows)
        def _(r):
            body(pl.ds(pl.multiple_of(r * step_rows, step_rows), step_rows), r)

    @pl.loop(0, total + 5 * LAG)
    def _(i):
        relayed, ended, swapped, passed, done = (i - k * LAG for k in range(1, 6))

        def at(q):
            return (q >= 0) & (q < total)

        @pl.when(middle & at(passed))
        def _():
            send_out(passed, theirs, far_send, far_sem, across).wait_recv()
            send_out(passed, theirs, pass_send, far_sem, near).start()

        @pl.when(middle & at(swapped))
        def _():
            @pl.when(swapped >= tiles)
            def _():
                send_swap(swapped).wait_recv()

            send_out(swapped, mine, near_send, near_sem, near).start()
            send_out(swapped, mine, far_send, far_sem, across).start()

        @pl.when(middle & at(relayed))
        def _():
            send_sums(relayed).wait_recv()
            base = lax.rem(col, 2) * half

            def body(_, r):
                lines = pl.ds(pl.multiple_of(base + r * step_rows, step_rows), step_rows)
                both = sums[relayed, lines, :].astype(jnp.float32)
                both += from_edge[relayed, lines, :].astype(jnp.float32)
                sums[relayed, lines, :] = both.astype(jnp.bfloat16)

            by_rows(half, body)
            send_relay(relayed).start()

        @pl.when(at(ended))
        def _():
            s, tile = split(ended)
            pltpu.make_async_copy(
                pre_ref.at[:, columns(place, tile)], pre.at[s, tile], pre_sem.at[ended]
            ).wait()

            @pl.when(middle)
            def _():
                send_relay(ended).wait_recv()
                base = lax.rem(col + 1, 2) * half

                def finish(r):
                    lines = pl.ds(pl.multiple_of(base + r * step_rows, step_rows), step_rows)
                    short = pl.ds(pl.multiple_of(r * step_rows, step_rows), step_rows)
                    back = sums[ended, lines, :].astype(jnp.float32)
                    back += from_edge[ended, lines, :].astype(jnp.float32)
                    back += from_middle[ended, short, :].astype(jnp.float32)
                    slope = gelu_slope(pre[s, tile, lines, :].astype(jnp.float32))
                    return lines, (back * slope).astype(jnp.bfloat16)

                @pl.when(ended < tiles)
                def _():
                    def body(_, r):
                        lines, value = finish(r)
                        out[place, tile, lines, :] = value

                    by_rows(half, body)

                @pl.when(ended >= tiles)
                def _():
                    def body(_, r):
                        lines, value = finish(r)
                        sums[ended, lines, :] = value

                    by_rows(half, body)
                    send_swap(ended).start()

        @pl.when(i < total)
        def _():
            s, tile = split(i)

            @pl.when(i < tiles)
            def _():
                load_weight(tile).wait()

            @pl.when((tile == 0) & (lax.rem(s, 2) == 1))
            def _():
                pltpu.make_async_copy(
                    grad_ref, grad.at[block_rows(s)], grad_sem.at[s]
                ).wait()

            sums[i] = lax.dot_general(
                grad[block_rows(s), :], weight[tile], (((1,), (1,)), ((), ())),
                preferred_element_type=jnp.float32,
            ).astype(jnp.bfloat16)

            @pl.when(edge)
            def _():
                send_sums(i).start()

        @pl.when(i < tiles)
        def _():
            send_pre(jnp.int32(1), i).start()

        turn = lax.div(i, 3) * 2 + lax.rem(i, 3)

        @pl.when((lax.rem(i, 3) < 2) & (turn < total - 2 * tiles))
        def _():
            s, tile = split(turn + 2 * tiles)
            send_pre(s, tile).start()

        @pl.when(i == tiles)
        def _():
            for s in range(2, depths, 2):
                send_grad(s).wait_recv()
                pass_grad(s).start()

        @pl.when(at(done))
        def _():
            @pl.when(edge)
            def _():
                send_out(done, theirs, near_send, near_sem, near).wait_recv()
                send_out(done, mine, far_send, far_sem, near).wait_recv()

            store_out(done).start()

        @pl.when(at(ended))
        def _():
            s, tile = split(ended)

            def body(lines, r):
                value = gelu_value(pre[s, tile, lines, :].astype(jnp.float32))
                where = pl.ds(pl.multiple_of(s * rows + r * step_rows, step_rows), step_rows)
                act[tile, where, :] = value.astype(jnp.bfloat16)

            by_rows(rows, body)

            @pl.when(ended >= total - tiles)
            def _():
                weight[tile] = lax.dot_general(
                    act[tile], grad[...], (((0,), (0,)), ((), ())),
                    preferred_element_type=jnp.float32,
                ).astype(jnp.bfloat16)
                store_gw(tile).start()

    pltpu.make_async_copy(weight, weight, gw_sem).wait()
    pltpu.make_async_copy(out, out, out_sem).wait()
    send_grad(1).wait_send()
    for s in range(2, depths, 2):
        send_grad(s).wait_send()
        pass_grad(s).wait_send()

    def drained(ref, sem):
        pltpu.make_async_copy(ref, ref, sem).wait()

    drained(pre.at[pl.ds(1, depths - 1)], pre_send)

    @pl.when(edge)
    def _():
        drained(sums, sums_send)

    @pl.when(middle)
    def _():
        drained(from_middle, relay_send)
        drained(from_middle.at[pl.ds(tiles, total - tiles)], swap_send)
        drained(from_middle, near_send)
        drained(from_middle, far_send)
        drained(from_middle, pass_send)


def solution(mesh):
    depths = mesh.shape["depth"]
    assert mesh.shape["col"] == 4

    def on_device(grad_out, pre_act, down_weight):
        rows, features = grad_out.shape
        hidden = down_weight.shape[0]
        width = 256 if hidden % 256 == 0 else 128
        tiles = hidden // width
        total = depths * tiles
        bf16 = jnp.bfloat16
        dma = pltpu.SemaphoreType.DMA
        anywhere = pl.BlockSpec(memory_space=pl.ANY)
        return pl.pallas_call(
            functools.partial(kernel, depths, width),
            out_shape=(
                jax.ShapeDtypeStruct(pre_act.shape, bf16),
                jax.ShapeDtypeStruct(down_weight.shape, bf16),
            ),
            in_specs=[anywhere] * 3,
            out_specs=(anywhere, anywhere),
            scratch_shapes=[
                pltpu.VMEM((total, rows, width), bf16),
                pltpu.VMEM((total, rows, width), bf16),
                pltpu.VMEM((total, rows // 2, width), bf16),
                pltpu.VMEM((depths, tiles, rows, width), bf16),
                pltpu.VMEM((tiles, depths * rows, width), bf16),
                pltpu.VMEM((depths, tiles, rows, width), bf16),
                pltpu.VMEM((tiles, width, features), bf16),
                pltpu.VMEM((depths * rows, features), bf16),
                dma((tiles,)), dma((total,)), dma((depths,)),
                dma((total,)), dma((total,)), dma((total,)), dma((total,)), dma((total,)),
                dma((depths,)), dma, dma, dma, dma, dma, dma, dma,
                dma, dma,
            ],
            compiler_params=pltpu.CompilerParams(
                collective_id=0, has_side_effects=True, vmem_limit_bytes=63 * 1024 * 1024
            ),
        )(grad_out, pre_act, down_weight)

    return jax.shard_map(
        on_device,
        mesh=mesh,
        in_specs=(P("depth", "col"), P("depth", "row"), P(("row", "depth"), "col")),
        out_specs=(P("depth", "row"), P(("row", "depth"), "col")),
        check_vma=False,
    )
```

```python
import functools

import jax
import jax.numpy as jnp
from jax import lax
from jax.experimental import pallas as pl
from jax.experimental.pallas import tpu as pltpu
from jax.sharding import PartitionSpec as P

MESH = pl.DeviceIdType.MESH
sqrt_two_pi = 0.7978845608028654
cubic_coeff = 0.044715
LAG = 2


def gelu_value(preact):
    tangent = jnp.tanh(sqrt_two_pi * (preact + cubic_coeff * preact * preact * preact))
    return 0.5 * preact * (1.0 + tangent)


def gelu_slope(preact):
    tangent = jnp.tanh(sqrt_two_pi * (preact + cubic_coeff * preact * preact * preact))
    inner = sqrt_two_pi * (1.0 + 3.0 * cubic_coeff * preact * preact)
    return 0.5 * (1.0 + tangent) + 0.5 * preact * (1.0 - tangent * tangent) * inner


def flip(a, b, extent):
    total, k = jnp.int32(0), 1
    while k < extent:
        bit = lax.div(a, jnp.int32(k)) + lax.div(b, jnp.int32(k))
        total = total + lax.rem(bit, jnp.int32(2)) * k
        k *= 2
    return total


def kernel(
    depths, width, grad_ref, pre_ref, weight_ref, out, weight,
    sums, from_edge, from_middle, pre, act, grad,
    weight_sem, pre_sem, grad_sem, edge_sem, middle_sem, swap_sem, near_sem, far_sem,
    grad_send, sums_send, relay_send, swap_send, near_send, far_send, pass_send, pre_send,
):
    col, place = lax.axis_index("col"), lax.axis_index("depth")
    rows, hidden = grad_ref.shape[0], weight_ref.shape[0]
    half = rows // 2
    tiles = hidden // width
    total = depths * tiles
    middle = (col == 1) | (col == 2)
    edge = (col == 0) | (col == 3)
    near = col + 1 - 2 * lax.rem(col, 2)
    across = 3 - col
    mine = pl.ds(pl.multiple_of(lax.rem(col + 1, 2) * half, half), half)
    theirs = pl.ds(pl.multiple_of(lax.rem(col, 2) * half, half), half)

    def columns(block, tile):
        return pl.ds(pl.multiple_of(block * hidden + tile * width, width), width)

    def to(axis, index):
        return {axis: index}

    def send(src, dst, send_sem, recv_sem, device):
        return pltpu.make_async_remote_copy(
            src_ref=src, dst_ref=dst, send_sem=send_sem, recv_sem=recv_sem,
            device_id=device, device_id_type=MESH,
        )

    def split(q):
        return lax.div(q, jnp.int32(tiles)), lax.rem(q, jnp.int32(tiles))

    def block_rows(s):
        return pl.ds(pl.multiple_of(s * rows, rows), rows)

    def tile_rows(tile):
        return pl.ds(pl.multiple_of(tile * width, width), width)

    def load_weight(tile):
        return pltpu.make_async_copy(
            weight_ref.at[tile_rows(tile), :], weight.at[tile_rows(tile), :], weight_sem.at[tile]
        )

    def load_pre(tile):
        return pltpu.make_async_copy(
            pre_ref.at[:, columns(place, tile)], pre.at[0, tile], pre_sem.at[tile]
        )

    def send_pre(s, tile):
        target = flip(place, s, depths)
        return send(
            pre_ref.at[:, columns(target, tile)], pre.at[s, tile], pre_send,
            pre_sem.at[s * tiles + tile], to("depth", target),
        )

    def load_grad():
        return pltpu.make_async_copy(grad_ref, grad.at[block_rows(0)], grad_sem.at[0])

    def send_grad(s):
        return send(
            grad_ref, grad.at[block_rows(s)], grad_send.at[s], grad_sem.at[s],
            to("depth", flip(place, jnp.int32(s), depths)),
        )

    def pass_grad(s):
        return send(
            grad.at[block_rows(s)], grad.at[block_rows(s + 1)], grad_send.at[s + 1],
            grad_sem.at[s + 1], to("depth", flip(place, jnp.int32(1), depths)),
        )

    def send_sums(q):
        return send(sums.at[q], from_edge.at[q], sums_send, edge_sem.at[q], to("col", near))

    def send_relay(q):
        return send(
            sums.at[q, theirs], from_middle.at[q], relay_send, middle_sem.at[q],
            to("col", across),
        )

    def send_swap(q):
        s, tile = split(q)
        return send(
            sums.at[q, mine], out.at[mine, columns(place, tile)], swap_send, swap_sem.at[q],
            to("depth", flip(place, s, depths)),
        )

    def send_out(q, which, send_sem, recv_sem, column):
        s, tile = split(q)
        part = out.at[which, columns(flip(place, s, depths), tile)]
        return send(part, part, send_sem, recv_sem.at[q], to("col", column))

    load_grad().start()
    load_weight(0).start()

    barrier = pltpu.get_barrier_semaphore()
    for s in range(1, depths):
        pl.semaphore_signal(
            barrier, inc=1, device_id=to("depth", flip(place, jnp.int32(s), depths)),
            device_id_type=MESH,
        )
    pl.semaphore_signal(barrier, inc=1, device_id=to("col", near), device_id_type=MESH)

    @pl.when(middle)
    def _():
        pl.semaphore_signal(barrier, inc=1, device_id=to("col", across), device_id_type=MESH)

    @pl.loop(1, tiles)
    def _(tile):
        load_weight(tile).start()

    @pl.loop(0, tiles)
    def _(tile):
        load_pre(tile).start()

    @pl.when(middle)
    def _():
        pl.semaphore_wait(barrier, depths + 1)

    @pl.when(edge)
    def _():
        pl.semaphore_wait(barrier, depths)

    send_grad(1).start()
    for s in range(2, depths, 2):
        send_grad(s).start()
    load_grad().wait()

    step_rows = 32

    def by_rows(count, body):
        @pl.loop(0, count // step_rows)
        def _(r):
            body(pl.ds(pl.multiple_of(r * step_rows, step_rows), step_rows), r)

    @pl.loop(0, total + 5 * LAG)
    def _(i):
        relayed, ended, swapped, passed, done = (i - k * LAG for k in range(1, 6))

        def at(q):
            return (q >= 0) & (q < total)

        @pl.when(middle & at(passed))
        def _():
            send_out(passed, theirs, far_send, far_sem, across).wait_recv()
            send_out(passed, theirs, pass_send, far_sem, near).start()

        @pl.when(middle & at(swapped))
        def _():
            @pl.when(swapped >= tiles)
            def _():
                send_swap(swapped).wait_recv()

            send_out(swapped, mine, near_send, near_sem, near).start()
            send_out(swapped, mine, far_send, far_sem, across).start()

        @pl.when(middle & at(relayed))
        def _():
            send_sums(relayed).wait_recv()
            base = lax.rem(col, 2) * half

            def body(_, r):
                lines = pl.ds(pl.multiple_of(base + r * step_rows, step_rows), step_rows)
                both = sums[relayed, lines, :].astype(jnp.float32)
                both += from_edge[relayed, lines, :].astype(jnp.float32)
                sums[relayed, lines, :] = both.astype(jnp.bfloat16)

            by_rows(half, body)
            send_relay(relayed).start()

        @pl.when(at(ended))
        def _():
            s, tile = split(ended)
            pltpu.make_async_copy(
                pre_ref.at[:, columns(place, tile)], pre.at[s, tile], pre_sem.at[ended]
            ).wait()

            @pl.when(middle)
            def _():
                send_relay(ended).wait_recv()
                base = lax.rem(col + 1, 2) * half

                def finish(r):
                    lines = pl.ds(pl.multiple_of(base + r * step_rows, step_rows), step_rows)
                    short = pl.ds(pl.multiple_of(r * step_rows, step_rows), step_rows)
                    back = sums[ended, lines, :].astype(jnp.float32)
                    back += from_edge[ended, lines, :].astype(jnp.float32)
                    back += from_middle[ended, short, :].astype(jnp.float32)
                    slope = gelu_slope(pre[s, tile, lines, :].astype(jnp.float32))
                    return lines, (back * slope).astype(jnp.bfloat16)

                @pl.when(ended < tiles)
                def _():
                    def body(_, r):
                        lines, value = finish(r)
                        out[lines, columns(place, tile)] = value

                    by_rows(half, body)

                @pl.when(ended >= tiles)
                def _():
                    def body(_, r):
                        lines, value = finish(r)
                        sums[ended, lines, :] = value

                    by_rows(half, body)
                    send_swap(ended).start()

        @pl.when(i < total)
        def _():
            s, tile = split(i)

            @pl.when(i < tiles)
            def _():
                load_weight(tile).wait()

            @pl.when((tile == 0) & (lax.rem(s, 2) == 1))
            def _():
                pltpu.make_async_copy(
                    grad_ref, grad.at[block_rows(s)], grad_sem.at[s]
                ).wait()

            sums[i] = lax.dot_general(
                grad[block_rows(s), :], weight[tile_rows(tile), :], (((1,), (1,)), ((), ())),
                preferred_element_type=jnp.float32,
            ).astype(jnp.bfloat16)

            @pl.when(edge)
            def _():
                send_sums(i).start()

        @pl.when(i < tiles)
        def _():
            send_pre(jnp.int32(1), i).start()

        turn = lax.div(i, 3) * 2 + lax.rem(i, 3)

        @pl.when((lax.rem(i, 3) < 2) & (turn < total - 2 * tiles))
        def _():
            s, tile = split(turn + 2 * tiles)
            send_pre(s, tile).start()

        @pl.when(i == tiles)
        def _():
            for s in range(2, depths, 2):
                send_grad(s).wait_recv()
                pass_grad(s).start()

        @pl.when(edge & at(done))
        def _():
            send_out(done, theirs, near_send, near_sem, near).wait_recv()
            send_out(done, mine, far_send, far_sem, near).wait_recv()

        @pl.when(at(ended))
        def _():
            s, tile = split(ended)

            def body(lines, r):
                value = gelu_value(pre[s, tile, lines, :].astype(jnp.float32))
                where = pl.ds(pl.multiple_of(s * rows + r * step_rows, step_rows), step_rows)
                act[tile, where, :] = value.astype(jnp.bfloat16)

            by_rows(rows, body)

            @pl.when(ended >= total - tiles)
            def _():
                weight[tile_rows(tile), :] = lax.dot_general(
                    act[tile], grad[...], (((0,), (0,)), ((), ())),
                    preferred_element_type=jnp.float32,
                ).astype(jnp.bfloat16)

    send_grad(1).wait_send()
    for s in range(2, depths, 2):
        send_grad(s).wait_send()
        pass_grad(s).wait_send()

    def drained(ref, sem):
        pltpu.make_async_copy(ref, ref, sem).wait()

    drained(pre.at[pl.ds(1, depths - 1)], pre_send)

    @pl.when(edge)
    def _():
        drained(sums, sums_send)

    @pl.when(middle)
    def _():
        drained(from_middle, relay_send)
        drained(from_middle.at[pl.ds(tiles, total - tiles)], swap_send)
        drained(from_middle, near_send)
        drained(from_middle, far_send)
        drained(from_middle, pass_send)


def solution(mesh):
    depths = mesh.shape["depth"]
    assert mesh.shape["col"] == 4

    def on_device(grad_out, pre_act, down_weight):
        rows, features = grad_out.shape
        hidden = down_weight.shape[0]
        width = 256 if hidden % 256 == 0 else 128
        tiles = hidden // width
        total = depths * tiles
        bf16 = jnp.bfloat16
        dma = pltpu.SemaphoreType.DMA
        anywhere = pl.BlockSpec(memory_space=pl.ANY)
        return pl.pallas_call(
            functools.partial(kernel, depths, width),
            out_shape=(
                pltpu.VMEM(pre_act.shape, bf16),
                pltpu.VMEM(down_weight.shape, bf16),
            ),
            in_specs=[anywhere] * 3,
            out_specs=(pl.BlockSpec(memory_space=pltpu.VMEM),) * 2,
            scratch_shapes=[
                pltpu.VMEM((total, rows, width), bf16),
                pltpu.VMEM((total, rows, width), bf16),
                pltpu.VMEM((total, rows // 2, width), bf16),
                pltpu.VMEM((depths, tiles, rows, width), bf16),
                pltpu.VMEM((tiles, depths * rows, width), bf16),
                pltpu.VMEM((depths * rows, features), bf16),
                dma((tiles,)), dma((total,)), dma((depths,)),
                dma((total,)), dma((total,)), dma((total,)), dma((total,)), dma((total,)),
                dma((depths,)), dma, dma, dma, dma, dma, dma, dma,
            ],
            compiler_params=pltpu.CompilerParams(
                collective_id=0, has_side_effects=True, vmem_limit_bytes=40 * 1024 * 1024
            ),
        )(grad_out, pre_act, down_weight)

    return jax.shard_map(
        on_device,
        mesh=mesh,
        in_specs=(P("depth", "col"), P("depth", "row"), P(("row", "depth"), "col")),
        out_specs=(P("depth", "row"), P(("row", "depth"), "col")),
        check_vma=False,
    )
```

```python
import functools

import jax
import jax.numpy as jnp
from jax import lax
from jax.experimental import pallas as pl
from jax.experimental.pallas import tpu as pltpu
from jax.sharding import PartitionSpec as P

MESH = pl.DeviceIdType.MESH
sqrt_two_pi = 0.7978845608028654
cubic_coeff = 0.044715
PARTS = 1
RELAY, PAIR, SWAP, PASS = 1, 1, 2, 1
TAIL = -(-(RELAY + 1) // PARTS)


def gelu_value(preact):
    tangent = jnp.tanh(sqrt_two_pi * (preact + cubic_coeff * preact * preact * preact))
    return 0.5 * preact * (1.0 + tangent)


def gelu_slope(preact):
    tangent = jnp.tanh(sqrt_two_pi * (preact + cubic_coeff * preact * preact * preact))
    inner = sqrt_two_pi * (1.0 + 3.0 * cubic_coeff * preact * preact)
    return 0.5 * (1.0 + tangent) + 0.5 * preact * (1.0 - tangent * tangent) * inner


def flip(a, b, extent):
    total, k = jnp.int32(0), 1
    while k < extent:
        bit = lax.div(a, jnp.int32(k)) + lax.div(b, jnp.int32(k))
        total = total + lax.rem(bit, jnp.int32(2)) * k
        k *= 2
    return total


def kernel(
    depths, width, grad_ref, pre_ref, weight_ref, out, weight,
    sums, from_edge, from_middle, pre, act, grad,
    weight_sem, pre_sem, grad_sem, edge_sem, middle_sem, swap_sem, far_sem, near_sem, pass_sem,
    grad_send, sums_send, relay_send, swap_send, near_send, far_send, pass_send, pre_send,
):
    col, place = lax.axis_index("col"), lax.axis_index("depth")
    rows, hidden = grad_ref.shape[0], weight_ref.shape[0]
    span = rows // PARTS
    half = span // 2
    tiles = hidden // width
    first = tiles - TAIL
    total = depths * tiles
    units = total * PARTS
    distant = total - 2 * tiles
    burst = 3 * distant // 4
    rest = max(burst, 2 * tiles)
    gap = max(g for g in (1, 2, 3) if rest + g * (distant - 1 - burst) < total - TAIL - 1 or g == 1)
    middle = (col == 1) | (col == 2)
    edge = (col == 0) | (col == 3)
    near = col + 1 - 2 * lax.rem(col, 2)
    across = 3 - col
    mine, theirs = lax.rem(col + 1, 2) * half, lax.rem(col, 2) * half

    def div(a, b):
        return lax.div(a, jnp.int32(b))

    def rem(a, b):
        return lax.rem(a, jnp.int32(b))

    def columns(block, tile):
        return pl.ds(pl.multiple_of(block * hidden + tile * width, width), width)

    def send(src, dst, send_sem, recv_sem, axis, index):
        return pltpu.make_async_remote_copy(
            src_ref=src, dst_ref=dst, send_sem=send_sem, recv_sem=recv_sem,
            device_id={axis: index}, device_id_type=MESH,
        )

    def block_tile(t):
        later = t - first + tiles
        others = (t >= first) & (t < total - TAIL)
        s = jnp.where(others, div(later, tiles), 0)
        tile = jnp.where(others, rem(later, tiles), jnp.where(t < first, t, t - total + tiles))
        return s, tile

    def unit(u):
        t = div(u, PARTS)
        s, tile = block_tile(t)
        return t, s, tile, rem(u, PARTS) * span

    def lines(start, count):
        return pl.ds(pl.multiple_of(start, count), count)

    def block_rows(s):
        return lines(s * rows, rows)

    def tile_rows(tile):
        return lines(tile * width, width)

    def load_weight(tile):
        return pltpu.make_async_copy(
            weight_ref.at[tile_rows(tile), :], weight.at[tile_rows(tile), :], weight_sem.at[tile]
        )

    def load_pre(s, tile):
        return pltpu.make_async_copy(
            pre_ref.at[:, columns(place, tile)], pre.at[s, tile], pre_sem.at[s * tiles + tile]
        )

    def send_pre(s, tile):
        target = flip(place, s, depths)
        return send(
            pre_ref.at[:, columns(target, tile)], pre.at[s, tile], pre_send,
            pre_sem.at[s * tiles + tile], "depth", target,
        )

    def load_grad(s):
        return pltpu.make_async_copy(grad_ref, grad.at[block_rows(s)], grad_sem.at[s])

    def send_grad(s):
        return send(
            grad_ref, grad.at[block_rows(s)], grad_send.at[s], grad_sem.at[s],
            "depth", flip(place, jnp.int32(s), depths),
        )

    def pass_grad(s):
        return send(
            grad.at[block_rows(s)], grad.at[block_rows(s + 1)], grad_send.at[s + 1],
            grad_sem.at[s + 1], "depth", flip(place, jnp.int32(1), depths),
        )

    def send_sums(u):
        t, _, _, base = unit(u)
        which = lines(base, span)
        return send(
            sums.at[t, which], from_edge.at[t, which], sums_send, edge_sem.at[u], "col", near
        )

    def send_relay(u):
        t, _, _, base = unit(u)
        return send(
            sums.at[t, lines(base + theirs, half)], from_middle.at[u], relay_send,
            middle_sem.at[u], "col", across,
        )

    def send_swap(u):
        t, s, tile, base = unit(u)
        which = lines(base + mine, half)
        return send(
            sums.at[t, which], out.at[which, columns(place, tile)], swap_send, swap_sem.at[u],
            "depth", flip(place, s, depths),
        )

    def send_out(u, part, send_sem, recv_sem, column):
        _, s, tile, base = unit(u)
        piece = out.at[lines(base + part, half), columns(flip(place, s, depths), tile)]
        return send(piece, piece, send_sem, recv_sem, "col", column)

    load_grad(0).start()
    load_weight(0).start()

    barrier = pltpu.get_barrier_semaphore()
    for s in range(1, depths):
        pl.semaphore_signal(
            barrier, inc=1, device_id={"depth": flip(place, jnp.int32(s), depths)},
            device_id_type=MESH,
        )
    pl.semaphore_signal(barrier, inc=1, device_id={"col": near}, device_id_type=MESH)

    @pl.when(middle)
    def _():
        pl.semaphore_signal(barrier, inc=1, device_id={"col": across}, device_id_type=MESH)

    @pl.loop(1, tiles)
    def _(tile):
        load_weight(tile).start()

    @pl.loop(0, tiles)
    def _(tile):
        load_pre(0, tile).start()

    @pl.when(middle)
    def _():
        pl.semaphore_wait(barrier, depths + 1)

    @pl.when(edge)
    def _():
        pl.semaphore_wait(barrier, depths)

    send_grad(1).start()
    for s in range(2, depths, 2):
        send_grad(s).start()
    load_grad(0).wait()

    step = 32

    def by_rows(count, body):
        @pl.loop(0, count // step)
        def _(r):
            body(r * step)

    def give_out(u):
        send_out(u, mine, near_send, near_sem, near).start()
        send_out(u, mine, far_send, far_sem.at[u], across).start()

    def pass_out(u):
        send_out(u, theirs, far_send, far_sem.at[u], across).wait_recv()
        send_out(u, theirs, pass_send, pass_sem, near).start()

    def own_tokens(u):
        return ((u >= 0) & (u < first * PARTS)) | ((u >= units - TAIL * PARTS) & (u < units))

    def pair_tokens(u):
        return (u >= first * PARTS) & (u < (first + tiles) * PARTS)

    def far_tokens(u):
        return (u >= (first + tiles) * PARTS) & (u < units - TAIL * PARTS)

    @pl.loop(0, units + 1 + RELAY + SWAP + PASS)
    def _(i):
        relayed = i - 1
        ended = relayed - RELAY
        @pl.when(middle & (relayed >= 0) & (relayed < units))
        def _():
            send_sums(relayed).wait_recv()
            t, _, _, base = unit(relayed)

            def body(r):
                which = lines(base + theirs + r, step)
                both = sums[t, which, :].astype(jnp.float32)
                both += from_edge[t, which, :].astype(jnp.float32)
                sums[t, which, :] = both.astype(jnp.bfloat16)

            by_rows(half, body)
            send_relay(relayed).start()

        @pl.when((ended >= 0) & (ended < units))
        def _():
            t, s, tile, base = unit(ended)

            @pl.when((s > 0) & (base == 0))
            def _():
                load_pre(s, tile).wait()

            @pl.when(middle)
            def _():
                send_relay(ended).wait_recv()

                def finish(r):
                    which = lines(base + mine + r, step)
                    back = sums[t, which, :].astype(jnp.float32)
                    back += from_edge[t, which, :].astype(jnp.float32)
                    back += from_middle[ended, lines(r, step), :].astype(jnp.float32)
                    slope = gelu_slope(pre[s, tile, which, :].astype(jnp.float32))
                    return which, (back * slope).astype(jnp.bfloat16)

                @pl.when(s == 0)
                def _():
                    def body(r):
                        which, value = finish(r)
                        out[which, columns(place, tile)] = value

                    by_rows(half, body)
                    give_out(ended)

                @pl.when(s > 0)
                def _():
                    def body(r):
                        which, value = finish(r)
                        sums[t, which, :] = value

                    by_rows(half, body)
                    send_swap(ended).start()

        @pl.when(middle & pair_tokens(ended - PAIR))
        def _():
            send_swap(ended - PAIR).wait_recv()
            give_out(ended - PAIR)

        @pl.when(middle & far_tokens(ended - SWAP))
        def _():
            send_swap(ended - SWAP).wait_recv()
            give_out(ended - SWAP)

        turn = div(i, PARTS)

        @pl.when((rem(i, PARTS) == 0) & (i < units))
        def _():
            s, tile = block_tile(turn)

            @pl.when((turn < first) | ((s == 1) & (tile >= first)))
            def _():
                load_weight(tile).wait()

            @pl.when((tile == 0) & (rem(s, 2) == 1))
            def _():
                load_grad(s).wait()

            sums[turn] = lax.dot_general(
                grad[block_rows(s), :], weight[tile_rows(tile), :], (((1,), (1,)), ((), ())),
                preferred_element_type=jnp.float32,
            ).astype(jnp.bfloat16)

            @pl.when(edge)
            def _():
                for part in range(PARTS):
                    send_sums(i + part).start()

            @pl.when(turn < tiles)
            def _():
                send_pre(jnp.int32(1), turn).start()

            def push(k):
                send_pre(2 + div(k, tiles), rem(k, tiles)).start()

            @pl.when(turn < burst)
            def _():
                push(turn)

            after = turn - rest
            slow = burst + div(after, gap)

            @pl.when((after >= 0) & (rem(after, gap) == 0) & (slow < distant))
            def _():
                push(slow)

            @pl.when(turn == tiles)
            def _():
                for s in range(2, depths, 2):
                    send_grad(s).wait_recv()
                    pass_grad(s).start()

            block, slot = div(turn, tiles), rem(turn, tiles)

            @pl.when(block == 0)
            def _():
                load_pre(0, slot).wait()

            def body(r):
                value = gelu_value(pre[block, slot, lines(r, step), :].astype(jnp.float32))
                act[slot, lines(block * rows + r, step), :] = value.astype(jnp.bfloat16)

            by_rows(rows, body)

            @pl.when(block == depths - 1)
            def _():
                weight[tile_rows(slot), :] = lax.dot_general(
                    act[slot], grad[...], (((0,), (0,)), ((), ())),
                    preferred_element_type=jnp.float32,
                ).astype(jnp.bfloat16)

        for among, lag in ((far_tokens, SWAP), (pair_tokens, PAIR), (own_tokens, 0)):
            @pl.when(middle & among(ended - lag - PASS))
            def _():
                pass_out(ended - lag - PASS)

    send_grad(1).wait_send()
    for s in range(2, depths, 2):
        send_grad(s).wait_send()
        pass_grad(s).wait_send()

    def drained(ref, sem):
        pltpu.make_async_copy(ref, ref, sem).wait()

    drained(pre.at[pl.ds(1, depths - 1)], pre_send)

    @pl.when(edge)
    def _():
        drained(sums, sums_send)
        drained(from_middle, near_sem)
        drained(from_middle, pass_sem)

    @pl.when(middle)
    def _():
        drained(from_middle, relay_send)
        drained(from_middle.at[pl.ds(0, units - tiles * PARTS)], swap_send)
        drained(from_middle, near_send)
        drained(from_middle, far_send)
        drained(from_middle, pass_send)


def write_out(results):
    parts = 4

    def body(first, second, first_out, second_out, sems):
        copies = []
        for k in range(parts):
            for n, (src, dst) in enumerate(((first, first_out), (second, second_out))):
                size = src.shape[0] // parts
                piece = pl.ds(k * size, size)
                copies.append(pltpu.make_async_copy(src.at[piece], dst.at[piece], sems.at[n, k]))
        for copy in copies:
            copy.start()
        for copy in copies:
            copy.wait()

    anywhere = pl.BlockSpec(memory_space=pl.ANY)
    return pl.pallas_call(
        body,
        out_shape=tuple(jax.ShapeDtypeStruct(r.shape, r.dtype) for r in results),
        in_specs=[pl.BlockSpec(memory_space=pltpu.VMEM)] * 2,
        out_specs=(anywhere, anywhere),
        scratch_shapes=[pltpu.SemaphoreType.DMA((2, parts))],
        compiler_params=pltpu.CompilerParams(vmem_limit_bytes=20 * 1024 * 1024),
    )(*results)


def solution(mesh):
    depths = mesh.shape["depth"]
    assert mesh.shape["col"] == 4

    def on_device(grad_out, pre_act, down_weight):
        rows, features = grad_out.shape
        hidden = down_weight.shape[0]
        width = 256 if hidden % 256 == 0 else 128
        tiles = hidden // width
        total = depths * tiles
        units = total * PARTS
        bf16 = jnp.bfloat16
        dma = pltpu.SemaphoreType.DMA
        anywhere = pl.BlockSpec(memory_space=pl.ANY)
        results = pl.pallas_call(
            functools.partial(kernel, depths, width),
            out_shape=(
                pltpu.VMEM(pre_act.shape, bf16),
                pltpu.VMEM(down_weight.shape, bf16),
            ),
            in_specs=[anywhere] * 3,
            out_specs=(pl.BlockSpec(memory_space=pltpu.VMEM),) * 2,
            scratch_shapes=[
                pltpu.VMEM((total, rows, width), bf16),
                pltpu.VMEM((total, rows, width), bf16),
                pltpu.VMEM((total * PARTS, rows // PARTS // 2, width), bf16),
                pltpu.VMEM((depths, tiles, rows, width), bf16),
                pltpu.VMEM((tiles, depths * rows, width), bf16),
                pltpu.VMEM((depths * rows, features), bf16),
                dma((tiles,)), dma((total,)), dma((depths,)),
                dma((units,)), dma((units,)), dma((units,)), dma((units,)), dma, dma,
                dma((depths,)), dma, dma, dma, dma, dma, dma, dma,
            ],
            compiler_params=pltpu.CompilerParams(
                collective_id=0, has_side_effects=True, vmem_limit_bytes=40 * 1024 * 1024
            ),
        )(grad_out, pre_act, down_weight)
        return write_out(results)

    return jax.shard_map(
        on_device,
        mesh=mesh,
        in_specs=(P("depth", "col"), P("depth", "row"), P(("row", "depth"), "col")),
        out_specs=(P("depth", "row"), P(("row", "depth"), "col")),
        check_vma=False,
    )
```

```python
import functools

import jax
import jax.numpy as jnp
from jax import lax
from jax.experimental import pallas as pl
from jax.experimental.pallas import tpu as pltpu
from jax.sharding import PartitionSpec as P

MESH = pl.DeviceIdType.MESH
sqrt_two_pi = 0.7978845608028654
cubic_coeff = 0.044715
HOP = 3
FINISH = 12


def gelu_value(preact):
    tangent = jnp.tanh(sqrt_two_pi * (preact + cubic_coeff * preact * preact * preact))
    return 0.5 * preact * (1.0 + tangent)


def gelu_slope(preact):
    tangent = jnp.tanh(sqrt_two_pi * (preact + cubic_coeff * preact * preact * preact))
    inner = sqrt_two_pi * (1.0 + 3.0 * cubic_coeff * preact * preact)
    return 0.5 * (1.0 + tangent) + 0.5 * preact * (1.0 - tangent * tangent) * inner


def flip(a, b, extent):
    total, k = jnp.int32(0), 1
    while k < extent:
        bit = lax.div(a, jnp.int32(k)) + lax.div(b, jnp.int32(k))
        total = total + lax.rem(bit, jnp.int32(2)) * k
        k *= 2
    return total


def kernel(
    depths, width, grad_ref, pre_ref, weight_ref, out, weight,
    sums, from_near, from_across, pre, act, grad,
    weight_sem, pre_sem, grad_sem, near_sem, across_sem, swap_sem, give_sem, far_sem, pass_sem,
    grad_send, near_send, across_send, swap_send, give_send, far_send, pass_send, pre_send,
):
    col, place = lax.axis_index("col"), lax.axis_index("depth")
    rows, hidden = grad_ref.shape[0], weight_ref.shape[0]
    half = rows // 2
    tiles = hidden // width
    total = depths * tiles
    middle = (col == 1) | (col == 2)
    edge = (col == 0) | (col == 3)
    near = col + 1 - 2 * lax.rem(col, 2)
    across = 3 - col
    mine = pl.multiple_of(lax.rem(col + 1, 2) * half, half)
    theirs = pl.multiple_of(lax.rem(col, 2) * half, half)

    def split(q):
        return lax.div(q, jnp.int32(tiles)), lax.rem(q, jnp.int32(tiles))

    def columns(block, tile):
        return pl.ds(pl.multiple_of(block * hidden + tile * width, width), width)

    def lines(start, count):
        return pl.ds(pl.multiple_of(start, count), count)

    def block_rows(s):
        return lines(s * rows, rows)

    def tile_rows(tile):
        return lines(tile * width, width)

    def send(src, dst, send_sem, recv_sem, axis, index):
        return pltpu.make_async_remote_copy(
            src_ref=src, dst_ref=dst, send_sem=send_sem, recv_sem=recv_sem,
            device_id={axis: index}, device_id_type=MESH,
        )

    def load_weight(tile):
        return pltpu.make_async_copy(
            weight_ref.at[tile_rows(tile), :], weight.at[tile_rows(tile), :], weight_sem.at[tile]
        )

    def load_pre(s, tile):
        return pltpu.make_async_copy(
            pre_ref.at[:, columns(place, tile)], pre.at[s, tile], pre_sem.at[s * tiles + tile]
        )

    def send_pre(s, tile):
        target = flip(place, s, depths)
        return send(
            pre_ref.at[:, columns(target, tile)], pre.at[s, tile], pre_send,
            pre_sem.at[s * tiles + tile], "depth", target,
        )

    def load_grad(s):
        return pltpu.make_async_copy(grad_ref, grad.at[block_rows(s)], grad_sem.at[s])

    def send_grad(s):
        return send(
            grad_ref, grad.at[block_rows(s)], grad_send.at[s], grad_sem.at[s],
            "depth", flip(place, jnp.int32(s), depths),
        )

    def pass_grad(s):
        return send(
            grad.at[block_rows(s)], grad.at[block_rows(s + 1)], grad_send.at[s + 1],
            grad_sem.at[s + 1], "depth", flip(place, jnp.int32(1), depths),
        )

    def send_near(q):
        return send(
            sums.at[q, lines(mine, half)], from_near.at[q], near_send, near_sem.at[q], "col", near
        )

    def send_across(q):
        return send(
            sums.at[q, lines(theirs, half)], from_across.at[q], across_send, across_sem.at[q],
            "col", across,
        )

    def send_swap(q):
        s, tile = split(q)
        which = lines(theirs, half)
        return send(
            sums.at[q, which], out.at[which, columns(place, tile)], swap_send, swap_sem.at[q],
            "depth", flip(place, s, depths),
        )

    def send_out(q, part, send_sem, recv_sem, column):
        s, tile = split(q)
        piece = out.at[lines(part, half), columns(flip(place, s, depths), tile)]
        return send(piece, piece, send_sem, recv_sem, "col", column)

    load_grad(0).start()
    load_weight(0).start()

    barrier = pltpu.get_barrier_semaphore()
    for s in range(1, depths):
        pl.semaphore_signal(
            barrier, inc=1, device_id={"depth": flip(place, jnp.int32(s), depths)},
            device_id_type=MESH,
        )
    pl.semaphore_signal(barrier, inc=1, device_id={"col": near}, device_id_type=MESH)

    @pl.when(middle)
    def _():
        pl.semaphore_signal(barrier, inc=1, device_id={"col": across}, device_id_type=MESH)

    @pl.loop(1, tiles)
    def _(tile):
        load_weight(tile).start()

    @pl.loop(0, tiles)
    def _(tile):
        load_pre(0, tile).start()

    @pl.when(middle)
    def _():
        pl.semaphore_wait(barrier, depths + 1)

    @pl.when(edge)
    def _():
        pl.semaphore_wait(barrier, depths)

    send_grad(1).start()
    for s in range(2, depths, 2):
        send_grad(s).start()
    load_grad(0).wait()

    step = 32

    def by_rows(count, body):
        @pl.loop(0, count // step)
        def _(r):
            body(r * step)

    def at(q):
        return (q >= 0) & (q < total)

    def add_into(q, part, other):
        def body(r):
            which = lines(part + r, step)
            both = sums[q, which, :].astype(jnp.float32)
            both += other[q, lines(r, step), :].astype(jnp.float32)
            sums[q, which, :] = both.astype(jnp.bfloat16)

        by_rows(half, body)

    turns = max(2 * total + 1 + HOP, total + FINISH + 2 * tiles)

    @pl.loop(0, turns)
    def _(i):
        inward = i - 1
        outward = inward - HOP
        ended = i - FINISH
        given = i - total
        spread = given - 1
        passed = spread - HOP

        @pl.when(middle & at(inward))
        def _():
            send_near(inward).wait_recv()
            add_into(inward, theirs, from_near)
            send_across(inward).start()

        @pl.when(middle & at(outward))
        def _():
            send_across(outward).wait_recv()
            add_into(outward, mine, from_across)
            send_near(outward).start()

        @pl.when(middle & at(spread))
        def _():
            send_out(spread, mine, give_send, give_sem.at[spread], near).wait_recv()
            send_out(spread, mine, far_send, far_sem.at[spread], across).start()

        @pl.when(middle & at(passed))
        def _():
            send_out(passed, theirs, far_send, far_sem.at[passed], across).wait_recv()
            send_out(passed, theirs, pass_send, pass_sem, near).start()

        @pl.when(edge & at(given))
        def _():
            @pl.when(given >= tiles)
            def _():
                send_swap(given).wait_recv()

            send_out(given, theirs, give_send, give_sem.at[given], near).start()

        @pl.when(i < total)
        def _():
            s, tile = split(i)

            @pl.when(s == 0)
            def _():
                load_weight(tile).wait()

            @pl.when((tile == 0) & (lax.rem(s, jnp.int32(2)) == 1))
            def _():
                load_grad(s).wait()

            sums[i] = lax.dot_general(
                grad[block_rows(s), :], weight[tile_rows(tile), :], (((1,), (1,)), ((), ())),
                preferred_element_type=jnp.float32,
            ).astype(jnp.bfloat16)

            @pl.when(edge)
            def _():
                send_near(i).start()

        @pl.when(i < tiles)
        def _():
            send_pre(jnp.int32(1), i).start()

        @pl.when(i < total - 2 * tiles)
        def _():
            s, tile = split(i)
            send_pre(s + 2, tile).start()

        @pl.when(i == tiles + tiles // 2)
        def _():
            for s in range(2, depths, 2):
                send_grad(s).wait_recv()
                pass_grad(s).start()

        @pl.when(at(ended))
        def _():
            s, tile = split(ended)
            load_pre(s, tile).wait()

            @pl.when(edge)
            def _():
                send_near(ended).wait_recv()

                def finish(r):
                    which = lines(theirs + r, step)
                    back = sums[ended, which, :].astype(jnp.float32)
                    back += from_near[ended, lines(r, step), :].astype(jnp.float32)
                    slope = gelu_slope(pre[s, tile, which, :].astype(jnp.float32))
                    return which, (back * slope).astype(jnp.bfloat16)

                @pl.when(s == 0)
                def _():
                    def body(r):
                        which, value = finish(r)
                        out[which, columns(place, tile)] = value

                    by_rows(half, body)

                @pl.when(s > 0)
                def _():
                    def body(r):
                        which, value = finish(r)
                        sums[ended, which, :] = value

                    by_rows(half, body)
                    send_swap(ended).start()

            def body(r):
                value = gelu_value(pre[s, tile, lines(r, step), :].astype(jnp.float32))
                act[tile, lines(s * rows + r, step), :] = value.astype(jnp.bfloat16)

            by_rows(rows, body)

        late = i - total - FINISH

        @pl.when((late >= 0) & (lax.rem(late, 2) == 0) & (late < 2 * tiles))
        def _():
            tile = lax.div(late, 2)
            weight[tile_rows(tile), :] = lax.dot_general(
                act[tile], grad[...], (((0,), (0,)), ((), ())),
                preferred_element_type=jnp.float32,
            ).astype(jnp.bfloat16)

    send_grad(1).wait_send()
    for s in range(2, depths, 2):
        send_grad(s).wait_send()
        pass_grad(s).wait_send()

    def drained(ref, sem):
        pltpu.make_async_copy(ref, ref, sem).wait()

    drained(pre.at[pl.ds(1, depths - 1)], pre_send)
    drained(from_near, near_send)

    @pl.when(edge)
    def _():
        drained(from_near.at[pl.ds(tiles, total - tiles)], swap_send)
        drained(from_near, give_send)
        drained(from_near, pass_sem)

    @pl.when(middle)
    def _():
        drained(from_near, across_send)
        drained(from_near, far_send)
        drained(from_near, pass_send)


def write_out(results):
    parts = 4

    def body(first, second, first_out, second_out, sems):
        copies = []
        for k in range(parts):
            for n, (src, dst) in enumerate(((first, first_out), (second, second_out))):
                size = src.shape[0] // parts
                piece = pl.ds(k * size, size)
                copies.append(pltpu.make_async_copy(src.at[piece], dst.at[piece], sems.at[n, k]))
        for copy in copies:
            copy.start()
        for copy in copies:
            copy.wait()

    anywhere = pl.BlockSpec(memory_space=pl.ANY)
    return pl.pallas_call(
        body,
        out_shape=tuple(jax.ShapeDtypeStruct(r.shape, r.dtype) for r in results),
        in_specs=[pl.BlockSpec(memory_space=pltpu.VMEM)] * 2,
        out_specs=(anywhere, anywhere),
        scratch_shapes=[pltpu.SemaphoreType.DMA((2, parts))],
        compiler_params=pltpu.CompilerParams(vmem_limit_bytes=20 * 1024 * 1024),
    )(*results)


def solution(mesh):
    depths = mesh.shape["depth"]
    assert mesh.shape["col"] == 4

    def on_device(grad_out, pre_act, down_weight):
        rows, features = grad_out.shape
        hidden = down_weight.shape[0]
        width = 256 if hidden % 256 == 0 else 128
        tiles = hidden // width
        total = depths * tiles
        bf16 = jnp.bfloat16
        dma = pltpu.SemaphoreType.DMA
        anywhere = pl.BlockSpec(memory_space=pl.ANY)
        results = pl.pallas_call(
            functools.partial(kernel, depths, width),
            out_shape=(
                pltpu.VMEM(pre_act.shape, bf16),
                pltpu.VMEM(down_weight.shape, bf16),
            ),
            in_specs=[anywhere] * 3,
            out_specs=(pl.BlockSpec(memory_space=pltpu.VMEM),) * 2,
            scratch_shapes=[
                pltpu.VMEM((total, rows, width), bf16),
                pltpu.VMEM((total, rows // 2, width), bf16),
                pltpu.VMEM((total, rows // 2, width), bf16),
                pltpu.VMEM((depths, tiles, rows, width), bf16),
                pltpu.VMEM((tiles, depths * rows, width), bf16),
                pltpu.VMEM((depths * rows, features), bf16),
                dma((tiles,)), dma((total,)), dma((depths,)),
                dma((total,)), dma((total,)), dma((total,)), dma((total,)), dma((total,)), dma,
                dma((depths,)), dma, dma, dma, dma, dma, dma, dma,
            ],
            compiler_params=pltpu.CompilerParams(
                collective_id=0, has_side_effects=True, vmem_limit_bytes=40 * 1024 * 1024
            ),
        )(grad_out, pre_act, down_weight)
        return write_out(results)

    return jax.shard_map(
        on_device,
        mesh=mesh,
        in_specs=(P("depth", "col"), P("depth", "row"), P(("row", "depth"), "col")),
        out_specs=(P("depth", "row"), P(("row", "depth"), "col")),
        check_vma=False,
    )
```

```python
import functools

import jax
import jax.numpy as jnp
from jax import lax
from jax.experimental import pallas as pl
from jax.experimental.pallas import tpu as pltpu
from jax.sharding import PartitionSpec as P

MESH = pl.DeviceIdType.MESH
sqrt_two_pi = 0.7978845608028654
cubic_coeff = 0.044715
HOP = 3
FINISH = 18
PIECES = 2


def gelu_value(preact):
    tangent = jnp.tanh(sqrt_two_pi * (preact + cubic_coeff * preact * preact * preact))
    return 0.5 * preact * (1.0 + tangent)


def gelu_slope(preact):
    tangent = jnp.tanh(sqrt_two_pi * (preact + cubic_coeff * preact * preact * preact))
    inner = sqrt_two_pi * (1.0 + 3.0 * cubic_coeff * preact * preact)
    return 0.5 * (1.0 + tangent) + 0.5 * preact * (1.0 - tangent * tangent) * inner


def flip(a, b, extent):
    total, k = jnp.int32(0), 1
    while k < extent:
        bit = lax.div(a, jnp.int32(k)) + lax.div(b, jnp.int32(k))
        total = total + lax.rem(bit, jnp.int32(2)) * k
        k *= 2
    return total


def kernel(
    depths, width, grad_ref, pre_ref, weight_ref, out, weight,
    sums, from_near, from_across, pre, act, grad,
    weight_sem, pre_sem, grad_sem, near_sem, across_sem, swap_sem, give_sem, far_sem, pass_sem,
    grad_send, near_send, across_send, swap_send, give_send, far_send, pass_send, pre_send,
):
    col, place = lax.axis_index("col"), lax.axis_index("depth")
    rows, hidden = grad_ref.shape[0], weight_ref.shape[0]
    half = rows // 2
    tiles = hidden // width
    total = depths * tiles
    middle = (col == 1) | (col == 2)
    edge = (col == 0) | (col == 3)
    near = col + 1 - 2 * lax.rem(col, 2)
    across = 3 - col
    mine = pl.multiple_of(lax.rem(col + 1, 2) * half, half)
    theirs = pl.multiple_of(lax.rem(col, 2) * half, half)

    def split(q):
        return lax.div(q, jnp.int32(tiles)), lax.rem(q, jnp.int32(tiles))

    def columns(block, tile):
        return pl.ds(pl.multiple_of(block * hidden + tile * width, width), width)

    def lines(start, count):
        return pl.ds(pl.multiple_of(start, count), count)

    def block_rows(s):
        return lines(s * rows, rows)

    def tile_rows(tile):
        return lines(tile * width, width)

    def send(src, dst, send_sem, recv_sem, axis, index):
        return pltpu.make_async_remote_copy(
            src_ref=src, dst_ref=dst, send_sem=send_sem, recv_sem=recv_sem,
            device_id={axis: index}, device_id_type=MESH,
        )

    def load_weight(tile):
        return pltpu.make_async_copy(
            weight_ref.at[tile_rows(tile), :], weight.at[tile_rows(tile), :], weight_sem.at[tile]
        )

    def load_pre(s, tile):
        return pltpu.make_async_copy(
            pre_ref.at[:, columns(place, tile)], pre.at[s, tile], pre_sem.at[s * tiles + tile]
        )

    def send_pre(s, tile):
        target = flip(place, s, depths)
        return send(
            pre_ref.at[:, columns(target, tile)], pre.at[s, tile], pre_send,
            pre_sem.at[s * tiles + tile], "depth", target,
        )

    def load_grad(s):
        return pltpu.make_async_copy(grad_ref, grad.at[block_rows(s)], grad_sem.at[s])

    def send_grad(s):
        return send(
            grad_ref, grad.at[block_rows(s)], grad_send.at[s], grad_sem.at[s],
            "depth", flip(place, jnp.int32(s), depths),
        )

    def pass_grad(s):
        return send(
            grad.at[block_rows(s)], grad.at[block_rows(s + 1)], grad_send.at[s + 1],
            grad_sem.at[s + 1], "depth", flip(place, jnp.int32(1), depths),
        )

    def send_near(q):
        return send(
            sums.at[q, lines(mine, half)], from_near.at[q], near_send, near_sem.at[q], "col", near
        )

    def send_across(q):
        return send(
            sums.at[q, lines(theirs, half)], from_across.at[q], across_send, across_sem.at[q],
            "col", across,
        )

    def send_swap(q):
        s, tile = split(q)
        which = lines(theirs, half)
        return send(
            sums.at[q, which], out.at[which, columns(place, tile)], swap_send, swap_sem.at[q],
            "depth", flip(place, s, depths),
        )

    def send_out(q, part, send_sem, recv_sem, column):
        s, tile = split(q)
        piece = out.at[lines(part, half), columns(flip(place, s, depths), tile)]
        return send(piece, piece, send_sem, recv_sem, "col", column)

    load_grad(0).start()
    load_weight(0).start()

    barrier = pltpu.get_barrier_semaphore()
    for s in range(1, depths):
        pl.semaphore_signal(
            barrier, inc=1, device_id={"depth": flip(place, jnp.int32(s), depths)},
            device_id_type=MESH,
        )
    pl.semaphore_signal(barrier, inc=1, device_id={"col": near}, device_id_type=MESH)

    @pl.when(middle)
    def _():
        pl.semaphore_signal(barrier, inc=1, device_id={"col": across}, device_id_type=MESH)

    @pl.loop(1, tiles)
    def _(tile):
        load_weight(tile).start()

    @pl.loop(0, tiles)
    def _(tile):
        load_pre(0, tile).start()

    @pl.when(middle)
    def _():
        pl.semaphore_wait(barrier, depths + 1)

    @pl.when(edge)
    def _():
        pl.semaphore_wait(barrier, depths)

    send_grad(1).start()
    for s in range(2, depths, 2):
        send_grad(s).start()
    load_grad(0).wait()

    step = 32

    def by_rows(count, body):
        @pl.loop(0, count // step)
        def _(r):
            body(r * step)

    def at(q):
        return (q >= 0) & (q < total)

    def add_into(q, part, other):
        def body(r):
            which = lines(part + r, step)
            both = sums[q, which, :].astype(jnp.float32)
            both += other[q, lines(r, step), :].astype(jnp.float32)
            sums[q, which, :] = both.astype(jnp.bfloat16)

        by_rows(half, body)

    turns = max(2 * total + 1 + HOP, total + FINISH + PIECES * tiles)

    @pl.loop(0, turns)
    def _(i):
        inward = i - 1
        outward = inward - HOP
        ended = i - FINISH
        given = i - total
        spread = given - 1
        passed = spread - HOP

        @pl.when(middle & at(inward))
        def _():
            send_near(inward).wait_recv()
            add_into(inward, theirs, from_near)
            send_across(inward).start()

        @pl.when(middle & at(outward))
        def _():
            send_across(outward).wait_recv()
            add_into(outward, mine, from_across)
            send_near(outward).start()

        @pl.when(middle & at(spread))
        def _():
            send_out(spread, mine, give_send, give_sem.at[spread], near).wait_recv()
            send_out(spread, mine, far_send, far_sem.at[spread], across).start()

        @pl.when(middle & at(passed))
        def _():
            send_out(passed, theirs, far_send, far_sem.at[passed], across).wait_recv()
            send_out(passed, theirs, pass_send, pass_sem, near).start()

        @pl.when(edge & at(given))
        def _():
            @pl.when(given >= tiles)
            def _():
                send_swap(given).wait_recv()

            send_out(given, theirs, give_send, give_sem.at[given], near).start()

        @pl.when(i < total)
        def _():
            s, tile = split(i)

            @pl.when(s == 0)
            def _():
                load_weight(tile).wait()

            @pl.when((tile == 0) & (lax.rem(s, jnp.int32(2)) == 1))
            def _():
                load_grad(s).wait()

            sums[i] = lax.dot_general(
                grad[block_rows(s), :], weight[tile_rows(tile), :], (((1,), (1,)), ((), ())),
                preferred_element_type=jnp.float32,
            ).astype(jnp.bfloat16)

            @pl.when(edge)
            def _():
                send_near(i).start()

        @pl.when(i < tiles)
        def _():
            send_pre(jnp.int32(1), i).start()

        @pl.when(i < total - 2 * tiles)
        def _():
            s, tile = split(i)
            send_pre(s + 2, tile).start()

        @pl.when(i == tiles + tiles // 2)
        def _():
            for s in range(2, depths, 2):
                send_grad(s).wait_recv()
                pass_grad(s).start()

        @pl.when(at(ended))
        def _():
            s, tile = split(ended)
            load_pre(s, tile).wait()

            @pl.when(edge)
            def _():
                send_near(ended).wait_recv()

                def finish(r):
                    which = lines(theirs + r, step)
                    back = sums[ended, which, :].astype(jnp.float32)
                    back += from_near[ended, lines(r, step), :].astype(jnp.float32)
                    slope = gelu_slope(pre[s, tile, which, :].astype(jnp.float32))
                    return which, (back * slope).astype(jnp.bfloat16)

                @pl.when(s == 0)
                def _():
                    def body(r):
                        which, value = finish(r)
                        out[which, columns(place, tile)] = value

                    by_rows(half, body)

                @pl.when(s > 0)
                def _():
                    def body(r):
                        which, value = finish(r)
                        sums[ended, which, :] = value

                    by_rows(half, body)
                    send_swap(ended).start()

            def body(r):
                value = gelu_value(pre[s, tile, lines(r, step), :].astype(jnp.float32))
                act[tile, lines(s * rows + r, step), :] = value.astype(jnp.bfloat16)

            by_rows(rows, body)

        late = i - total - FINISH

        @pl.when((late >= 0) & (late < PIECES * tiles))
        def _():
            tile = lax.div(late, jnp.int32(PIECES))
            size = weight.shape[1] // PIECES
            which = lines(lax.rem(late, jnp.int32(PIECES)) * size, size)
            weight[tile_rows(tile), which] = lax.dot_general(
                act[tile], grad[:, which], (((0,), (0,)), ((), ())),
                preferred_element_type=jnp.float32,
            ).astype(jnp.bfloat16)

    send_grad(1).wait_send()
    for s in range(2, depths, 2):
        send_grad(s).wait_send()
        pass_grad(s).wait_send()

    def drained(ref, sem):
        pltpu.make_async_copy(ref, ref, sem).wait()

    drained(pre.at[pl.ds(1, depths - 1)], pre_send)
    drained(from_near, near_send)

    @pl.when(edge)
    def _():
        drained(from_near.at[pl.ds(tiles, total - tiles)], swap_send)
        drained(from_near, give_send)
        drained(from_near, pass_sem)

    @pl.when(middle)
    def _():
        drained(from_near, across_send)
        drained(from_near, far_send)
        drained(from_near, pass_send)


def write_out(results):
    parts = 16

    def body(first, second, first_out, second_out, sems):
        copies = []
        for k in range(parts):
            for n, (src, dst) in enumerate(((first, first_out), (second, second_out))):
                size = src.shape[0] // parts
                piece = pl.ds(k * size, size)
                copies.append(pltpu.make_async_copy(src.at[piece], dst.at[piece], sems.at[n, k]))
        for copy in copies:
            copy.start()
        for copy in copies:
            copy.wait()

    anywhere = pl.BlockSpec(memory_space=pl.ANY)
    return pl.pallas_call(
        body,
        out_shape=tuple(jax.ShapeDtypeStruct(r.shape, r.dtype) for r in results),
        in_specs=[pl.BlockSpec(memory_space=pltpu.VMEM)] * 2,
        out_specs=(anywhere, anywhere),
        scratch_shapes=[pltpu.SemaphoreType.DMA((2, parts))],
        compiler_params=pltpu.CompilerParams(vmem_limit_bytes=20 * 1024 * 1024),
    )(*results)


def solution(mesh):
    depths = mesh.shape["depth"]
    assert mesh.shape["col"] == 4

    def on_device(grad_out, pre_act, down_weight):
        rows, features = grad_out.shape
        hidden = down_weight.shape[0]
        width = 256 if hidden % 256 == 0 else 128
        tiles = hidden // width
        total = depths * tiles
        bf16 = jnp.bfloat16
        dma = pltpu.SemaphoreType.DMA
        anywhere = pl.BlockSpec(memory_space=pl.ANY)
        results = pl.pallas_call(
            functools.partial(kernel, depths, width),
            out_shape=(
                pltpu.VMEM(pre_act.shape, bf16),
                pltpu.VMEM(down_weight.shape, bf16),
            ),
            in_specs=[anywhere] * 3,
            out_specs=(pl.BlockSpec(memory_space=pltpu.VMEM),) * 2,
            scratch_shapes=[
                pltpu.VMEM((total, rows, width), bf16),
                pltpu.VMEM((total, rows // 2, width), bf16),
                pltpu.VMEM((total, rows // 2, width), bf16),
                pltpu.VMEM((depths, tiles, rows, width), bf16),
                pltpu.VMEM((tiles, depths * rows, width), bf16),
                pltpu.VMEM((depths * rows, features), bf16),
                dma((tiles,)), dma((total,)), dma((depths,)),
                dma((total,)), dma((total,)), dma((total,)), dma((total,)), dma((total,)), dma,
                dma((depths,)), dma, dma, dma, dma, dma, dma, dma,
            ],
            compiler_params=pltpu.CompilerParams(
                collective_id=0, has_side_effects=True, vmem_limit_bytes=40 * 1024 * 1024
            ),
        )(grad_out, pre_act, down_weight)
        return write_out(results)

    return jax.shard_map(
        on_device,
        mesh=mesh,
        in_specs=(P("depth", "col"), P("depth", "row"), P(("row", "depth"), "col")),
        out_specs=(P("depth", "row"), P(("row", "depth"), "col")),
        check_vma=False,
    )
```

```python
import functools

import jax
import jax.numpy as jnp
from jax import lax
from jax.experimental import pallas as pl
from jax.experimental.pallas import tpu as pltpu
from jax.sharding import PartitionSpec as P

MESH = pl.DeviceIdType.MESH
sqrt_two_pi = 0.7978845608028654
cubic_coeff = 0.044715
HOP = 3
FINISH = 18
PIECES = 2


def gelu_value(preact):
    tangent = jnp.tanh(sqrt_two_pi * (preact + cubic_coeff * preact * preact * preact))
    return 0.5 * preact * (1.0 + tangent)


def gelu_slope(preact):
    tangent = jnp.tanh(sqrt_two_pi * (preact + cubic_coeff * preact * preact * preact))
    inner = sqrt_two_pi * (1.0 + 3.0 * cubic_coeff * preact * preact)
    return 0.5 * (1.0 + tangent) + 0.5 * preact * (1.0 - tangent * tangent) * inner


def flip(a, b, extent):
    total, k = jnp.int32(0), 1
    while k < extent:
        bit = lax.div(a, jnp.int32(k)) + lax.div(b, jnp.int32(k))
        total = total + lax.rem(bit, jnp.int32(2)) * k
        k *= 2
    return total


def kernel(
    depths, width, grad_ref, pre_ref, weight_ref, out, weight,
    sums, from_near, from_across, pre, act, grad,
    weight_sem, pre_sem, grad_sem, near_sem, across_sem, swap_sem, give_sem, far_sem, pass_sem,
    grad_send, near_send, across_send, swap_send, give_send, far_send, pass_send, pre_send,
):
    col, place = lax.axis_index("col"), lax.axis_index("depth")
    rows, hidden = grad_ref.shape[0], weight_ref.shape[0]
    half = rows // 2
    tiles = hidden // width
    total = depths * tiles
    middle = (col == 1) | (col == 2)
    edge = (col == 0) | (col == 3)
    near = col + 1 - 2 * lax.rem(col, 2)
    across = 3 - col
    mine = pl.multiple_of(lax.rem(col + 1, 2) * half, half)
    theirs = pl.multiple_of(lax.rem(col, 2) * half, half)

    def split(q):
        return lax.div(q, jnp.int32(tiles)), lax.rem(q, jnp.int32(tiles))

    def columns(block, tile):
        return pl.ds(pl.multiple_of(block * hidden + tile * width, width), width)

    def lines(start, count):
        return pl.ds(pl.multiple_of(start, count), count)

    def block_rows(s):
        return lines(s * rows, rows)

    def tile_rows(tile):
        return lines(tile * width, width)

    def send(src, dst, send_sem, recv_sem, axis, index):
        return pltpu.make_async_remote_copy(
            src_ref=src, dst_ref=dst, send_sem=send_sem, recv_sem=recv_sem,
            device_id={axis: index}, device_id_type=MESH,
        )

    def load_weight(tile):
        return pltpu.make_async_copy(
            weight_ref.at[tile_rows(tile), :], weight.at[tile_rows(tile), :], weight_sem.at[tile]
        )

    def load_pre(s, tile):
        return pltpu.make_async_copy(
            pre_ref.at[:, columns(place, tile)], pre.at[s, tile], pre_sem.at[s * tiles + tile]
        )

    def send_pre(s, tile):
        target = flip(place, s, depths)
        return send(
            pre_ref.at[:, columns(target, tile)], pre.at[s, tile], pre_send,
            pre_sem.at[s * tiles + tile], "depth", target,
        )

    def load_grad(s):
        return pltpu.make_async_copy(grad_ref, grad.at[block_rows(s)], grad_sem.at[s])

    def send_grad(s):
        return send(
            grad_ref, grad.at[block_rows(s)], grad_send.at[s], grad_sem.at[s],
            "depth", flip(place, jnp.int32(s), depths),
        )

    def pass_grad(s):
        return send(
            grad.at[block_rows(s)], grad.at[block_rows(s + 1)], grad_send.at[s + 1],
            grad_sem.at[s + 1], "depth", flip(place, jnp.int32(1), depths),
        )

    def send_near(q):
        return send(
            sums.at[q, lines(mine, half)], from_near.at[q], near_send, near_sem.at[q], "col", near
        )

    def send_across(q):
        return send(
            sums.at[q, lines(theirs, half)], from_across.at[q], across_send, across_sem.at[q],
            "col", across,
        )

    def send_swap(q):
        s, tile = split(q)
        which = lines(theirs, half)
        return send(
            sums.at[q, which], out.at[which, columns(place, tile)], swap_send, swap_sem.at[q],
            "depth", flip(place, s, depths),
        )

    def send_out(q, part, send_sem, recv_sem, column):
        s, tile = split(q)
        piece = out.at[lines(part, half), columns(flip(place, s, depths), tile)]
        return send(piece, piece, send_sem, recv_sem, "col", column)

    load_grad(0).start()
    load_weight(0).start()

    barrier = pltpu.get_barrier_semaphore()
    for s in range(1, depths):
        pl.semaphore_signal(
            barrier, inc=1, device_id={"depth": flip(place, jnp.int32(s), depths)},
            device_id_type=MESH,
        )
    pl.semaphore_signal(barrier, inc=1, device_id={"col": near}, device_id_type=MESH)

    @pl.when(middle)
    def _():
        pl.semaphore_signal(barrier, inc=1, device_id={"col": across}, device_id_type=MESH)

    @pl.loop(1, tiles)
    def _(tile):
        load_weight(tile).start()

    @pl.loop(0, tiles)
    def _(tile):
        load_pre(0, tile).start()

    @pl.when(middle)
    def _():
        pl.semaphore_wait(barrier, depths + 1)

    @pl.when(edge)
    def _():
        pl.semaphore_wait(barrier, depths)

    send_grad(1).start()
    for s in range(2, depths, 2):
        send_grad(s).start()
    load_grad(0).wait()

    step = 64

    def by_rows(count, body):
        @pl.loop(0, count // step)
        def _(r):
            body(r * step)

    def at(q):
        return (q >= 0) & (q < total)

    def add_into(q, part, other):
        def body(r):
            which = lines(part + r, step)
            both = sums[q, which, :].astype(jnp.float32)
            both += other[q, lines(r, step), :].astype(jnp.float32)
            sums[q, which, :] = both.astype(jnp.bfloat16)

        by_rows(half, body)

    finish_lag = min(FINISH, total - 1)
    turns = max(2 * total + 1 + HOP, total + finish_lag + PIECES * tiles)

    @pl.loop(0, turns)
    def _(i):
        inward = i - 1
        outward = inward - HOP
        ended = i - finish_lag
        given = i - total
        spread = given - 1
        passed = spread - HOP

        @pl.when(middle & at(inward))
        def _():
            send_near(inward).wait_recv()
            add_into(inward, theirs, from_near)
            send_across(inward).start()

        @pl.when(middle & at(outward))
        def _():
            send_across(outward).wait_recv()
            add_into(outward, mine, from_across)
            send_near(outward).start()

        @pl.when(middle & at(spread))
        def _():
            send_out(spread, mine, give_send, give_sem.at[spread], near).wait_recv()
            send_out(spread, mine, far_send, far_sem.at[spread], across).start()

        @pl.when(middle & at(passed))
        def _():
            send_out(passed, theirs, far_send, far_sem.at[passed], across).wait_recv()
            send_out(passed, theirs, pass_send, pass_sem, near).start()

        @pl.when(edge & at(given))
        def _():
            @pl.when(given >= tiles)
            def _():
                send_swap(given).wait_recv()

            send_out(given, theirs, give_send, give_sem.at[given], near).start()

        @pl.when(i < total)
        def _():
            s, tile = split(i)

            @pl.when(s == 0)
            def _():
                load_weight(tile).wait()

            @pl.when((tile == 0) & (lax.rem(s, jnp.int32(2)) == 1))
            def _():
                load_grad(s).wait()

            sums[i] = lax.dot_general(
                grad[block_rows(s), :], weight[tile_rows(tile), :], (((1,), (1,)), ((), ())),
                preferred_element_type=jnp.float32,
            ).astype(jnp.bfloat16)

            @pl.when(edge)
            def _():
                send_near(i).start()

        @pl.when(i < tiles)
        def _():
            send_pre(jnp.int32(1), i).start()

        @pl.when(i < total - 2 * tiles)
        def _():
            s, tile = split(i)
            send_pre(s + 2, tile).start()

        @pl.when(i == tiles + tiles // 2)
        def _():
            for s in range(2, depths, 2):
                send_grad(s).wait_recv()
                pass_grad(s).start()

        @pl.when(at(ended))
        def _():
            s, tile = split(ended)
            load_pre(s, tile).wait()

            @pl.when(edge)
            def _():
                send_near(ended).wait_recv()

                def finish(r):
                    which = lines(theirs + r, step)
                    back = sums[ended, which, :].astype(jnp.float32)
                    back += from_near[ended, lines(r, step), :].astype(jnp.float32)
                    slope = gelu_slope(pre[s, tile, which, :].astype(jnp.float32))
                    return which, (back * slope).astype(jnp.bfloat16)

                @pl.when(s == 0)
                def _():
                    def body(r):
                        which, value = finish(r)
                        out[which, columns(place, tile)] = value

                    by_rows(half, body)

                @pl.when(s > 0)
                def _():
                    def body(r):
                        which, value = finish(r)
                        sums[ended, which, :] = value

                    by_rows(half, body)
                    send_swap(ended).start()

            def body(r):
                value = gelu_value(pre[s, tile, lines(r, step), :].astype(jnp.float32))
                act[tile, lines(s * rows + r, step), :] = value.astype(jnp.bfloat16)

            by_rows(rows, body)

        late = i - total - finish_lag

        @pl.when((late >= 0) & (late < PIECES * tiles))
        def _():
            tile = lax.div(late, jnp.int32(PIECES))
            size = weight.shape[1] // PIECES
            which = lines(lax.rem(late, jnp.int32(PIECES)) * size, size)
            weight[tile_rows(tile), which] = lax.dot_general(
                act[tile], grad[:, which], (((0,), (0,)), ((), ())),
                preferred_element_type=jnp.float32,
            ).astype(jnp.bfloat16)

    send_grad(1).wait_send()
    for s in range(2, depths, 2):
        send_grad(s).wait_send()
        pass_grad(s).wait_send()

    def drained(ref, sem):
        pltpu.make_async_copy(ref, ref, sem).wait()

    drained(pre.at[pl.ds(1, depths - 1)], pre_send)
    drained(from_near, near_send)

    @pl.when(edge)
    def _():
        drained(from_near.at[pl.ds(tiles, total - tiles)], swap_send)
        drained(from_near, give_send)
        drained(from_near, pass_sem)

    @pl.when(middle)
    def _():
        drained(from_near, across_send)
        drained(from_near, far_send)
        drained(from_near, pass_send)


def write_out(results):
    parts = 16

    def body(first, second, first_out, second_out, sems):
        copies = []
        for k in range(parts):
            for n, (src, dst) in enumerate(((first, first_out), (second, second_out))):
                size = src.shape[0] // parts
                piece = pl.ds(k * size, size)
                copies.append(pltpu.make_async_copy(src.at[piece], dst.at[piece], sems.at[n, k]))
        for copy in copies:
            copy.start()
        for copy in copies:
            copy.wait()

    anywhere = pl.BlockSpec(memory_space=pl.ANY)
    return pl.pallas_call(
        body,
        out_shape=tuple(jax.ShapeDtypeStruct(r.shape, r.dtype) for r in results),
        in_specs=[pl.BlockSpec(memory_space=pltpu.VMEM)] * 2,
        out_specs=(anywhere, anywhere),
        scratch_shapes=[pltpu.SemaphoreType.DMA((2, parts))],
        compiler_params=pltpu.CompilerParams(vmem_limit_bytes=20 * 1024 * 1024),
    )(*results)


def solution(mesh):
    depths = mesh.shape["depth"]
    assert mesh.shape["col"] == 4

    def on_device(grad_out, pre_act, down_weight):
        rows, features = grad_out.shape
        hidden = down_weight.shape[0]
        width = 256 if hidden % 256 == 0 else 128
        tiles = hidden // width
        total = depths * tiles
        bf16 = jnp.bfloat16
        dma = pltpu.SemaphoreType.DMA
        anywhere = pl.BlockSpec(memory_space=pl.ANY)
        results = pl.pallas_call(
            functools.partial(kernel, depths, width),
            out_shape=(
                pltpu.VMEM(pre_act.shape, bf16),
                pltpu.VMEM(down_weight.shape, bf16),
            ),
            in_specs=[anywhere] * 3,
            out_specs=(pl.BlockSpec(memory_space=pltpu.VMEM),) * 2,
            scratch_shapes=[
                pltpu.VMEM((total, rows, width), bf16),
                pltpu.VMEM((total, rows // 2, width), bf16),
                pltpu.VMEM((total, rows // 2, width), bf16),
                pltpu.VMEM((depths, tiles, rows, width), bf16),
                pltpu.VMEM((tiles, depths * rows, width), bf16),
                pltpu.VMEM((depths * rows, features), bf16),
                dma((tiles,)), dma((total,)), dma((depths,)),
                dma((total,)), dma((total,)), dma((total,)), dma((total,)), dma((total,)), dma,
                dma((depths,)), dma, dma, dma, dma, dma, dma, dma,
            ],
            compiler_params=pltpu.CompilerParams(
                collective_id=0, has_side_effects=True, vmem_limit_bytes=40 * 1024 * 1024
            ),
        )(grad_out, pre_act, down_weight)
        return write_out(results)

    return jax.shard_map(
        on_device,
        mesh=mesh,
        in_specs=(P("depth", "col"), P("depth", "row"), P(("row", "depth"), "col")),
        out_specs=(P("depth", "row"), P(("row", "depth"), "col")),
        check_vma=False,
    )
```

```python
import functools

import jax
import jax.numpy as jnp
from jax import lax
from jax.experimental import pallas as pl
from jax.experimental.pallas import tpu as pltpu
from jax.sharding import PartitionSpec as P

MESH = pl.DeviceIdType.MESH
sqrt_two_pi = 0.7978845608028654
cubic_coeff = 0.044715
HOP = 3
FINISH = 18
PIECES = 2


def gelu_value(preact):
    tangent = jnp.tanh(sqrt_two_pi * (preact + cubic_coeff * preact * preact * preact))
    return 0.5 * preact * (1.0 + tangent)


def gelu_slope(preact):
    tangent = jnp.tanh(sqrt_two_pi * (preact + cubic_coeff * preact * preact * preact))
    inner = sqrt_two_pi * (1.0 + 3.0 * cubic_coeff * preact * preact)
    return 0.5 * (1.0 + tangent) + 0.5 * preact * (1.0 - tangent * tangent) * inner


def flip(a, b, extent):
    total, k = jnp.int32(0), 1
    while k < extent:
        bit = lax.div(a, jnp.int32(k)) + lax.div(b, jnp.int32(k))
        total = total + lax.rem(bit, jnp.int32(2)) * k
        k *= 2
    return total


def kernel(
    depths, width, grad_ref, pre_ref, weight_ref, out, weight,
    sums, from_near, from_across, pre, act, grad,
    weight_sem, pre_sem, grad_sem, near_sem, across_sem, swap_sem, give_sem, far_sem, pass_sem,
    grad_send, near_send, across_send, swap_send, give_send, far_send, pass_send, pre_send,
):
    col, place = lax.axis_index("col"), lax.axis_index("depth")
    rows, hidden = grad_ref.shape[0], weight_ref.shape[0]
    half = rows // 2
    tiles = hidden // width
    total = depths * tiles
    middle = (col == 1) | (col == 2)
    edge = (col == 0) | (col == 3)
    near = col + 1 - 2 * lax.rem(col, 2)
    across = 3 - col
    mine = pl.multiple_of(lax.rem(col + 1, 2) * half, half)
    theirs = pl.multiple_of(lax.rem(col, 2) * half, half)

    def split(q):
        return lax.div(q, jnp.int32(tiles)), lax.rem(q, jnp.int32(tiles))

    def columns(block, tile):
        return pl.ds(pl.multiple_of(block * hidden + tile * width, width), width)

    def lines(start, count):
        return pl.ds(pl.multiple_of(start, count), count)

    def block_rows(s):
        return lines(s * rows, rows)

    def tile_rows(tile):
        return lines(tile * width, width)

    def send(src, dst, send_sem, recv_sem, axis, index):
        return pltpu.make_async_remote_copy(
            src_ref=src, dst_ref=dst, send_sem=send_sem, recv_sem=recv_sem,
            device_id={axis: index}, device_id_type=MESH,
        )

    def load_weight(tile):
        return pltpu.make_async_copy(
            weight_ref.at[tile_rows(tile), :], weight.at[tile_rows(tile), :], weight_sem.at[tile]
        )

    def load_pre(s, tile):
        return pltpu.make_async_copy(
            pre_ref.at[:, columns(place, tile)], pre.at[s, tile], pre_sem.at[s * tiles + tile]
        )

    def send_pre(s, tile):
        target = flip(place, s, depths)
        return send(
            pre_ref.at[:, columns(target, tile)], pre.at[s, tile], pre_send,
            pre_sem.at[s * tiles + tile], "depth", target,
        )

    def load_grad(s):
        return pltpu.make_async_copy(grad_ref, grad.at[block_rows(s)], grad_sem.at[s])

    def send_grad(s):
        return send(
            grad_ref, grad.at[block_rows(s)], grad_send.at[s], grad_sem.at[s],
            "depth", flip(place, jnp.int32(s), depths),
        )

    def pass_grad(s):
        return send(
            grad.at[block_rows(s)], grad.at[block_rows(s + 1)], grad_send.at[s + 1],
            grad_sem.at[s + 1], "depth", flip(place, jnp.int32(1), depths),
        )

    def send_near(q):
        return send(
            sums.at[q, lines(mine, half)], from_near.at[q], near_send, near_sem.at[q], "col", near
        )

    def send_across(q):
        return send(
            sums.at[q, lines(theirs, half)], from_across.at[q], across_send, across_sem.at[q],
            "col", across,
        )

    def send_swap(q):
        s, tile = split(q)
        which = lines(theirs, half)
        return send(
            sums.at[q, which], out.at[which, columns(place, tile)], swap_send, swap_sem.at[q],
            "depth", flip(place, s, depths),
        )

    def send_out(q, part, send_sem, recv_sem, column):
        s, tile = split(q)
        piece = out.at[lines(part, half), columns(flip(place, s, depths), tile)]
        return send(piece, piece, send_sem, recv_sem, "col", column)

    load_grad(0).start()
    load_weight(0).start()

    barrier = pltpu.get_barrier_semaphore()
    for s in range(1, depths):
        pl.semaphore_signal(
            barrier, inc=1, device_id={"depth": flip(place, jnp.int32(s), depths)},
            device_id_type=MESH,
        )
    pl.semaphore_signal(barrier, inc=1, device_id={"col": near}, device_id_type=MESH)

    @pl.when(middle)
    def _():
        pl.semaphore_signal(barrier, inc=1, device_id={"col": across}, device_id_type=MESH)

    @pl.loop(1, tiles)
    def _(tile):
        load_weight(tile).start()

    @pl.loop(0, tiles)
    def _(tile):
        load_pre(0, tile).start()

    @pl.when(middle)
    def _():
        pl.semaphore_wait(barrier, depths + 1)

    @pl.when(edge)
    def _():
        pl.semaphore_wait(barrier, depths)

    send_grad(1).start()
    for s in range(2, depths, 2):
        send_grad(s).start()
    load_grad(0).wait()

    step = 32

    def by_rows(count, body):
        @pl.loop(0, count // step)
        def _(r):
            body(r * step)

    def at(q):
        return (q >= 0) & (q < total)

    def add_into(q, part, other):
        def body(r):
            which = lines(part + r, step)
            both = sums[q, which, :].astype(jnp.float32)
            both += other[q, lines(r, step), :].astype(jnp.float32)
            sums[q, which, :] = both.astype(jnp.bfloat16)

        by_rows(half, body)

    turns = max(2 * total + 1 + HOP, total + FINISH + PIECES * tiles)

    @pl.loop(0, turns)
    def _(i):
        inward = i - 1
        outward = inward - HOP
        ended = i - FINISH
        given = i - total
        spread = given - 1
        passed = spread - HOP

        @pl.when(middle & at(inward))
        def _():
            send_near(inward).wait_recv()
            add_into(inward, theirs, from_near)
            send_across(inward).start()

        @pl.when(middle & at(outward))
        def _():
            send_across(outward).wait_recv()
            add_into(outward, mine, from_across)
            send_near(outward).start()

        @pl.when(middle & at(spread))
        def _():
            send_out(spread, mine, give_send, give_sem.at[spread], near).wait_recv()
            send_out(spread, mine, far_send, far_sem.at[spread], across).start()

        @pl.when(middle & at(passed))
        def _():
            send_out(passed, theirs, far_send, far_sem.at[passed], across).wait_recv()
            send_out(passed, theirs, pass_send, pass_sem, near).start()

        @pl.when(edge & at(given))
        def _():
            @pl.when(given >= tiles)
            def _():
                send_swap(given).wait_recv()

            send_out(given, theirs, give_send, give_sem.at[given], near).start()

        @pl.when(i < total)
        def _():
            s, tile = split(i)

            @pl.when(s == 0)
            def _():
                load_weight(tile).wait()

            @pl.when((tile == 0) & (lax.rem(s, jnp.int32(2)) == 1))
            def _():
                load_grad(s).wait()

            sums[i] = lax.dot_general(
                grad[block_rows(s), :], weight[tile_rows(tile), :], (((1,), (1,)), ((), ())),
                preferred_element_type=jnp.float32,
            ).astype(jnp.bfloat16)

            @pl.when(edge)
            def _():
                send_near(i).start()

        @pl.when(i < tiles)
        def _():
            send_pre(jnp.int32(1), i).start()

        @pl.when(i < total - 2 * tiles)
        def _():
            s, tile = split(i)
            send_pre(s + 2, tile).start()

        @pl.when(i == tiles + tiles // 2)
        def _():
            for s in range(2, depths, 2):
                send_grad(s).wait_recv()
                pass_grad(s).start()

        @pl.when(at(ended))
        def _():
            s, tile = split(ended)
            load_pre(s, tile).wait()

            @pl.when(edge)
            def _():
                send_near(ended).wait_recv()

                def finish(r):
                    which = lines(theirs + r, step)
                    back = sums[ended, which, :].astype(jnp.float32)
                    back += from_near[ended, lines(r, step), :].astype(jnp.float32)
                    slope = gelu_slope(pre[s, tile, which, :].astype(jnp.float32))
                    return which, (back * slope).astype(jnp.bfloat16)

                @pl.when(s == 0)
                def _():
                    def body(r):
                        which, value = finish(r)
                        out[which, columns(place, tile)] = value

                    by_rows(half, body)

                @pl.when(s > 0)
                def _():
                    def body(r):
                        which, value = finish(r)
                        sums[ended, which, :] = value

                    by_rows(half, body)
                    send_swap(ended).start()

            def body(r):
                value = gelu_value(pre[s, tile, lines(r, step), :].astype(jnp.float32))
                act[tile, lines(s * rows + r, step), :] = value.astype(jnp.bfloat16)

            by_rows(rows, body)

        late = i - total - FINISH

        @pl.when((late >= 0) & (late < PIECES * tiles))
        def _():
            tile = lax.div(late, jnp.int32(PIECES))
            size = weight.shape[1] // PIECES
            which = lines(lax.rem(late, jnp.int32(PIECES)) * size, size)
            weight[tile_rows(tile), which] = lax.dot_general(
                act[tile], grad[:, which], (((0,), (0,)), ((), ())),
                preferred_element_type=jnp.float32,
            ).astype(jnp.bfloat16)

    send_grad(1).wait_send()
    for s in range(2, depths, 2):
        send_grad(s).wait_send()
        pass_grad(s).wait_send()

    def drained(ref, sem):
        pltpu.make_async_copy(ref, ref, sem).wait()

    drained(pre.at[pl.ds(1, depths - 1)], pre_send)
    drained(from_near, near_send)

    @pl.when(edge)
    def _():
        drained(from_near.at[pl.ds(tiles, total - tiles)], swap_send)
        drained(from_near, give_send)
        drained(from_near, pass_sem)

    @pl.when(middle)
    def _():
        drained(from_near, across_send)
        drained(from_near, far_send)
        drained(from_near, pass_send)


def write_out(results):
    parts = 16

    def body(first, second, first_out, second_out, sems):
        copies = []
        for k in range(parts):
            for n, (src, dst) in enumerate(((first, first_out), (second, second_out))):
                size = src.shape[0] // parts
                piece = pl.ds(k * size, size)
                copies.append(pltpu.make_async_copy(src.at[piece], dst.at[piece], sems.at[n, k]))
        for k, copy in enumerate(copies):
            copy.start(priority=k % 2)
        for copy in copies:
            copy.wait()

    anywhere = pl.BlockSpec(memory_space=pl.ANY)
    return pl.pallas_call(
        body,
        out_shape=tuple(jax.ShapeDtypeStruct(r.shape, r.dtype) for r in results),
        in_specs=[pl.BlockSpec(memory_space=pltpu.VMEM)] * 2,
        out_specs=(anywhere, anywhere),
        scratch_shapes=[pltpu.SemaphoreType.DMA((2, parts))],
        compiler_params=pltpu.CompilerParams(vmem_limit_bytes=20 * 1024 * 1024),
    )(*results)


def solution(mesh):
    depths = mesh.shape["depth"]
    assert mesh.shape["col"] == 4

    def on_device(grad_out, pre_act, down_weight):
        rows, features = grad_out.shape
        hidden = down_weight.shape[0]
        width = 256 if hidden % 256 == 0 else 128
        tiles = hidden // width
        total = depths * tiles
        bf16 = jnp.bfloat16
        dma = pltpu.SemaphoreType.DMA
        anywhere = pl.BlockSpec(memory_space=pl.ANY)
        results = pl.pallas_call(
            functools.partial(kernel, depths, width),
            out_shape=(
                pltpu.VMEM(pre_act.shape, bf16),
                pltpu.VMEM(down_weight.shape, bf16),
            ),
            in_specs=[anywhere] * 3,
            out_specs=(pl.BlockSpec(memory_space=pltpu.VMEM),) * 2,
            scratch_shapes=[
                pltpu.VMEM((total, rows, width), bf16),
                pltpu.VMEM((total, rows // 2, width), bf16),
                pltpu.VMEM((total, rows // 2, width), bf16),
                pltpu.VMEM((depths, tiles, rows, width), bf16),
                pltpu.VMEM((tiles, depths * rows, width), bf16),
                pltpu.VMEM((depths * rows, features), bf16),
                dma((tiles,)), dma((total,)), dma((depths,)),
                dma((total,)), dma((total,)), dma((total,)), dma((total,)), dma((total,)), dma,
                dma((depths,)), dma, dma, dma, dma, dma, dma, dma,
            ],
            compiler_params=pltpu.CompilerParams(
                collective_id=0, has_side_effects=True, vmem_limit_bytes=40 * 1024 * 1024
            ),
        )(grad_out, pre_act, down_weight)
        return write_out(results)

    return jax.shard_map(
        on_device,
        mesh=mesh,
        in_specs=(P("depth", "col"), P("depth", "row"), P(("row", "depth"), "col")),
        out_specs=(P("depth", "row"), P(("row", "depth"), "col")),
        check_vma=False,
    )
```
